32 devices in a mesh: lat: 16 (over z, y, x), head: 2 (over core).
Axes of the slice: x: 2, y: 2, z: 4, core: 2. Of those that a mesh axis runs over, the one named last changes fastest.
Arguments:
- grid_latent: bfloat16 [131072, 512], P('lat'), may hold values from -6 to 6
- mesh_latent: bfloat16 [10240, 512], P('lat'), may hold values from -6 to 6
- neighbours: int32 [10240, 16], P('lat'), may hold values from -1 to 131071, as said below
- edge_bias: bfloat16 [10240, 64], P('lat', 'head'), may hold values from -8 to 384
- query_weight: bfloat16 [512, 512], P(None, 'head'), may hold values from -0.25 to 0.25
- key_weight: bfloat16 [512, 512], P(None, 'head'), may hold values from -0.25 to 0.25
- value_weight: bfloat16 [512, 512], P(None, 'head'), may hold values from -0.25 to 0.25
- out_weight: bfloat16 [512, 512], P('head'), may hold values from -0.25 to 0.25
- norm_gain: bfloat16 [512], P('head'), may hold values from 0.5 to 1.5
Outputs:
- mesh_out: bfloat16 [10240, 512], P('lat', 'head')
The draws below stay inside these ranges and needn't reach their ends.
Inputs may be any that keep to these rules, and one draw needn't show every extreme that they name: `neighbours`: every neighbour of mesh node m is -1 or lies in [b * 8192 - 2048, (b + 1) * 8192 + 2048) with b = m // 640; both ends of that range (cut to the grid) are named in every draw; slots 0 and 1 are never -1.
All inputs are finite; a program needn't handle non-finite values.
Results may differ from the reference program's by a relative error of at most 0.0075.
Values may be sent and summed in bfloat16 or wider, within the bound.
A program may use at most 128 MiB of HBM per device.

```python
import math
import jax
import jax.numpy as jnp
from jax import lax

D = 512
HEADS = 4
K = 16
G_DEV = 8192
M_DEV = 640
HEAD_DIM = 128
HALO = 2048
GRID = 131072
MESH = 10240


def draw_neighbours(key, part):
    mesh_ids = jnp.arange(MESH, dtype=jnp.int32)
    owner = mesh_ids // M_DEV
    lowest = jnp.maximum(owner * G_DEV - HALO, 0)
    highest = jnp.minimum((owner + 1) * G_DEV + HALO, GRID)
    key_pick = jax.random.fold_in(key, 11)
    key_pad = jax.random.fold_in(key, 23)
    offsets = jax.random.randint(key_pick, (MESH, K), 0, (highest - lowest)[:, None])
    picked = lowest[:, None] + offsets
    first = (mesh_ids % M_DEV == 0)[:, None]
    slot = jnp.arange(K, dtype=jnp.int32)[None, :]
    picked = jnp.where(first & (slot == 0), lowest[:, None], picked)
    picked = jnp.where(first & (slot == 1), highest[:, None] - 1, picked)
    padded = (jax.random.randint(key_pad, (MESH, K), 0, 4) == 0) & (slot >= 2)
    return jnp.where(padded, -1, picked).astype(jnp.int32)


def draw_edge_bias(key, part):
    base = jnp.clip(jax.random.normal(jax.random.fold_in(key, 37), (MESH, HEADS * K), jnp.float32), -8.0, 8.0)
    return base.astype(jnp.bfloat16)


def shard_levels(key, extent, cuts, smallest, high):
    def one(dim, shards_of):
        steps = jax.random.uniform(jax.random.fold_in(jax.random.fold_in(key, 6), dim), (shards_of,), jnp.float32, smallest / len(cuts), high / len(cuts))
        return jnp.repeat(jnp.exp(steps), extent[dim] // shards_of).reshape((-1,) + (1,) * (len(extent) - dim - 1))

    level = one(*cuts[0])
    for cut in cuts[1:]:
        level = level * one(*cut)
    return level


def gaussian(key, dims, deviation, limit, shards=(), kind=jnp.bfloat16):
    array = jax.random.normal(key, dims, jnp.float32) * deviation
    if len(shards) > 0:
        array = shard_levels(key, dims, shards, -0.22, 0.18) * array
    return jnp.clip(array, min=-limit, max=limit).astype(kind)


def setup_inputs(seed: int = 0) -> dict:
    splits = jax.random.split(jax.random.key(seed), 10)
    grid_latent = gaussian(splits[0], (GRID, D), 1.0, 6.0, ((0, 16),))
    mesh_latent = gaussian(splits[1], (MESH, D), 1.0, 6.0, ((0, 16),))
    neighbours = draw_neighbours(jax.random.fold_in(splits[9], 71), 0)
    edge_bias = draw_edge_bias(jax.random.fold_in(splits[9], 71), 0)
    query_weight = gaussian(splits[4], (D, D), D ** -0.5, 0.25, ((1, 2),))
    key_weight = gaussian(splits[5], (D, D), D ** -0.5, 0.25, ((1, 2),))
    value_weight = gaussian(splits[6], (D, D), D ** -0.5, 0.25, ((1, 2),))
    out_weight = gaussian(splits[7], (D, D), D ** -0.5, 0.25, ((0, 2),))
    norm_gain = jnp.clip(1.0 + 0.1 * jax.random.normal(splits[8], (D,), jnp.float32), 0.5, 1.5).astype(jnp.bfloat16)
    return dict(grid_latent=grid_latent, mesh_latent=mesh_latent, neighbours=neighbours, edge_bias=edge_bias, query_weight=query_weight, key_weight=key_weight, value_weight=value_weight, out_weight=out_weight, norm_gain=norm_gain)


EPSILON = 1e-05

def reference(grid_latent, mesh_latent, neighbours, edge_bias, query_weight, key_weight, value_weight, out_weight, norm_gain):

    def attend_block(blocks):
        mesh_rows, neigh_rows, bias_rows = blocks
        count = mesh_rows.shape[0]
        queries = jnp.dot(mesh_rows, query_weight, preferred_element_type=jnp.float32).astype(jnp.bfloat16)
        valid = neigh_rows >= 0
        safe_index = jnp.where(valid, neigh_rows, 0).astype(jnp.int32)
        fetched = grid_latent[safe_index.reshape(-1)]
        keys = jnp.dot(fetched, key_weight, preferred_element_type=jnp.float32).astype(jnp.bfloat16)
        values = jnp.dot(fetched, value_weight, preferred_element_type=jnp.float32).astype(jnp.bfloat16)
        keys = keys.reshape(count, K, HEADS, HEAD_DIM).astype(jnp.float32)
        values = values.reshape(count, K, HEADS, HEAD_DIM).astype(jnp.float32)
        query_heads = queries.astype(jnp.float32).reshape(count, HEADS, HEAD_DIM)
        scores = jnp.einsum('bhc,bkhc->bhk', query_heads, keys) * HEAD_DIM ** (-0.5)
        scores = scores + bias_rows.astype(jnp.float32).reshape(count, HEADS, K)
        live = valid[:, None, :]
        scores = jnp.where(live, scores, -1e+30)
        top_score = lax.optimization_barrier(jnp.max(scores, axis=2, keepdims=True))
        weights = jnp.where(live, jnp.exp(scores - top_score), 0.0)
        total = lax.optimization_barrier(jnp.sum(weights, axis=2))
        mixed = jnp.einsum('bhk,bkhc->bhc', weights, values) / total[:, :, None]
        attended = mixed.reshape(count, D).astype(jnp.bfloat16)
        projected = jnp.dot(attended, out_weight, preferred_element_type=jnp.float32)
        updated = mesh_rows.astype(jnp.float32) + projected
        mean = lax.optimization_barrier(jnp.sum(updated, axis=1)) / D
        variance = lax.optimization_barrier(jnp.sum(updated * updated, axis=1)) / D - mean * mean
        normed = (updated - mean[:, None]) * lax.rsqrt(variance[:, None] + EPSILON) * norm_gain.astype(jnp.float32)
        return normed.astype(jnp.bfloat16)
    block = math.gcd(MESH, 512)
    nblocks = MESH // block
    result = lax.map(attend_block, (mesh_latent.reshape(nblocks, block, D), neighbours.reshape(nblocks, block, K), edge_bias.reshape(nblocks, block, HEADS * K)))
    return result.reshape(MESH, D)
```

```python
import functools

import jax
import jax.numpy as jnp
from jax import lax
from jax.experimental import pallas as pl
from jax.experimental.pallas import tpu as pltpu
from jax.sharding import PartitionSpec as P

HEAD_DIM = 128
LANES = 128
SUB = 8
EPSILON = 1e-05
DEAD = -1e30
PIECE = 1024
GROUP = 8
MESH = pl.DeviceIdType.MESH

WEIGHTS = 0
OWN_BIAS = 5
REQUEST = 6
REQUEST_COPIES = 4


def body(
    order_own, order_send, bias_send, grid_in, mesh_in, query_in, key_in, value_in, out_in, gain_in,
    out_ref,
    wide, stage, picked, query_w, key_w, value_w, out_w, gain,
    nodes, order_land, order_low, order_high, bias_land, bias_rows,
    fold, fold_own, mixed, mixed_own, lse, lse_own,
    partial, partial_lse, reply, reply_lse, normed,
    stage_sems, local_sems, order_sems, send_sems, recv_sems,
):
    band, width = grid_in.shape
    part = nodes.shape[1]
    heads = width // HEAD_DIM
    split = heads // 2
    cols = width // LANES
    side = width // 2
    chunks = order_own.shape[0]
    chunk_rows = LANES * cols
    padded = lse.shape[1]
    reply_base = REQUEST + 2 * REQUEST_COPIES
    last_copy = reply_base + 2 * (heads + 1)

    lat = lax.axis_index("lat")
    me = lax.axis_index("head")
    size = lax.axis_size("lat")
    other = 1 - me
    above = lax.rem(lat + 1, size)
    below = lax.rem(lat + size - 1, size)
    partner = (lat, other)

    def fetch(n):
        return pltpu.make_async_copy(
            grid_in.at[pl.ds(n * PIECE, PIECE)], stage.at[n % 2], stage_sems.at[n % 2]
        )

    fetch(0).start()
    fetch(1).start()
    mine = [
        pltpu.make_async_copy(src, dst, local_sems.at[n])
        for n, (src, dst) in enumerate((
            (query_in, query_w.at[me]),
            (key_in, key_w.at[me]),
            (value_in, value_w.at[me]),
            (out_in, out_w.at[pl.ds(me * side, side)]),
            (gain_in, gain.at[me]),
            (bias_send.at[2, me], bias_land.at[2, me]),
            (mesh_in.at[pl.ds(me * part, part)], nodes.at[2]),
        ))
    ]
    for copy in mine:
        copy.start()

    barrier = pltpu.get_barrier_semaphore()
    peers = (partner, (above, me), (below, me), (above, other), (below, other))
    for peer in peers:
        pl.semaphore_signal(barrier, inc=1, device_id=peer, device_id_type=MESH)
    pl.semaphore_wait(barrier, len(peers))

    def remote(n, src, dst, device):
        return pltpu.make_async_remote_copy(
            src_ref=src, dst_ref=dst, send_sem=send_sems.at[n], recv_sem=recv_sems.at[n],
            device_id=device, device_id_type=MESH,
        )

    requests = []
    for s, target in enumerate((above, below)):
        at = REQUEST + s * REQUEST_COPIES
        requests.append((
            remote(at, order_send.at[s], order_land.at[s], (target, me)),
            remote(at + 1, bias_send.at[s, me], bias_land.at[s, me], (target, me)),
            remote(at + 2, bias_send.at[s, other], bias_land.at[s, me], (target, other)),
            remote(at + 3, mesh_in.at[pl.ds(me * part, part)], nodes.at[s], (target, me)),
        ))
    shared = [
        remote(WEIGHTS, query_in, query_w.at[me], partner),
        remote(WEIGHTS + 1, key_in, key_w.at[me], partner),
        remote(WEIGHTS + 2, value_in, value_w.at[me], partner),
        remote(WEIGHTS + 3, out_in, out_w.at[pl.ds(me * side, side)], partner),
        remote(WEIGHTS + 4, gain_in, gain.at[me], partner),
        remote(OWN_BIAS, bias_send.at[2, other], bias_land.at[2, me], partner),
    ]
    for copy in requests[0]:
        copy.start()
    for copy in shared:
        copy.start()
    for copy in requests[1]:
        copy.start()

    lse[...] = jnp.zeros(lse.shape, jnp.float32)

    pieces = band // PIECE
    for n in range(pieces):
        fetch(n).wait()

        def widen(step, carry, n=n):
            row = pl.multiple_of(step * 32, 32)
            block = stage[n % 2, pl.ds(row, 32), :].astype(jnp.float32)
            for t in range(4):
                for c in range(cols):
                    at = n * PIECE * cols + row * cols + (t * cols + c) * SUB
                    wide[pl.ds(pl.multiple_of(at, SUB), SUB), :] = block[
                        t * SUB : (t + 1) * SUB, c * LANES : (c + 1) * LANES
                    ]
            return carry

        lax.fori_loop(0, PIECE // 32, widen, 0)
        if n + 2 < pieces:
            fetch(n + 2).start()

    diagonal = (
        lax.broadcasted_iota(jnp.int32, (SUB, LANES), 1) // (LANES // SUB)
        == lax.broadcasted_iota(jnp.int32, (SUB, LANES), 0)
    )
    lane = lax.broadcasted_iota(jnp.int32, (padded, LANES), 1)

    def project(s, fold_ref):
        rows = nodes[s]
        for half in range(2):
            queries = jnp.dot(
                rows, query_w[half], preferred_element_type=jnp.float32
            ).astype(jnp.bfloat16)
            for h in range(split):
                span = slice(h * HEAD_DIM, (h + 1) * HEAD_DIM)
                fold_ref[half * split + h] = lax.dot_general(
                    queries[:, span], key_w[half, :, span],
                    (((1,), (1,)), ((), ())), preferred_element_type=jnp.float32,
                )
        bias_rows[...] = jnp.concatenate(
            [bias_land[s, half].astype(jnp.float32) for half in range(2)], axis=0
        )

    def gather(order, chunk, u):
        for e in range(LANES):
            at = order[chunk, e]
            to = u * chunk_rows + (e // SUB) * (cols * SUB) + e % SUB
            picked[pl.ds(to, cols, stride=SUB), :] = wide[pl.ds(at, cols, stride=SUB), :]

    def score(fold_ref, mixed_ref, lse_ref, chunk, u):
        start = u * chunk_rows
        rows = jnp.concatenate(
            [
                jnp.concatenate(
                    [
                        picked[start + (t * cols + c) * SUB : start + (t * cols + c + 1) * SUB, :]
                        for t in range(LANES // SUB)
                    ],
                    axis=0,
                ).astype(jnp.bfloat16)
                for c in range(cols)
            ],
            axis=1,
        )
        at = pl.ds(pl.multiple_of(chunk * SUB, SUB), SUB)
        left = jnp.concatenate([fold_ref[h, at, :] for h in range(heads)], axis=0)
        scores = lax.dot_general(
            left.astype(jnp.bfloat16), rows,
            (((1,), (1,)), ((), ())), preferred_element_type=jnp.float32,
        )
        bias = jnp.concatenate(
            [
                jnp.where(diagonal, bias_rows[pl.ds(h * chunks + chunk, 1), :], DEAD)
                for h in range(heads)
            ],
            axis=0,
        )
        scores = scores * HEAD_DIM ** (-0.5) + bias
        top = jnp.max(scores, axis=1, keepdims=True)
        weights = jnp.exp(scores - top)
        total = jnp.sum(weights, axis=1, keepdims=True)
        summed = jnp.dot(
            weights.astype(jnp.bfloat16), rows, preferred_element_type=jnp.float32
        ) * (1.0 / total)
        level = jnp.broadcast_to(top + jnp.log(total), (heads * SUB, LANES))
        for h in range(heads):
            mixed_ref[h, at, :] = summed[h * SUB : (h + 1) * SUB]
            lse_ref[h, at, :] = level[h * SUB : (h + 1) * SUB]

    def run(order, fold_ref, mixed_ref, lse_ref, low, high):
        for u in range(GROUP):
            gather(order, low + u, u)

        def step(n, carry):
            chunk = low + n * GROUP
            after = lax.rem(chunk + GROUP, chunks)
            for u in range(GROUP):
                score(fold_ref, mixed_ref, lse_ref, chunk + u, u)
            for u in range(GROUP):
                gather(order, after + u, u)
            return carry

        lax.fori_loop(0, (high - low) // GROUP, step, 0)

    def values(mixed_ref, h):
        half, inner = h // split, h % split
        return jnp.dot(
            mixed_ref[h].astype(jnp.bfloat16),
            value_w[half, :, inner * HEAD_DIM : (inner + 1) * HEAD_DIM],
            preferred_element_type=jnp.float32,
        )

    for copy in mine:
        copy.wait()
    for copy in shared:
        copy.wait_recv()
    project(2, fold_own)
    first = (chunks // GROUP // 2) * GROUP
    run(order_own, fold_own, mixed_own, lse_own, 0, first)

    replies = []
    for s, (target, order) in enumerate(((below, order_low), (above, order_high))):
        order_copy = pltpu.make_async_copy(order_land.at[s], order, order_sems.at[s])
        requests[s][0].wait_recv()
        order_copy.start()
        for copy in requests[s][1:]:
            copy.wait_recv()
        project(s, fold)
        order_copy.wait()
        run(order, fold, mixed, lse, 0, chunks)
        sends = [
            remote(reply_base + s * (heads + 1) + h, partial.at[s, h], reply.at[s, h], (target, me))
            for h in range(heads)
        ] + [
            remote(
                reply_base + s * (heads + 1) + heads, partial_lse.at[s], reply_lse.at[s],
                (target, me),
            )
        ]
        level = lse[0]
        for h in range(1, heads):
            level = jnp.where(lane == h, lse[h], level)
        for b in range(padded // LANES):
            partial_lse[s, :, b * LANES : (b + 1) * LANES] = level[
                b * LANES : (b + 1) * LANES
            ].T[:SUB]
        for h in range(heads):
            partial[s, h] = values(mixed, h).astype(jnp.bfloat16)
            if h == 0:
                sends[heads].start()
            else:
                sends[h - 1].start()
        sends[heads - 1].start()
        replies.append(sends)

    project_bias = jnp.concatenate(
        [bias_land[2, half].astype(jnp.float32) for half in range(2)], axis=0
    )
    bias_rows[...] = project_bias
    run(order_own, fold_own, mixed_own, lse_own, first, chunks)

    for sends in replies:
        for copy in sends:
            copy.wait_recv()
    filler = jnp.zeros((LANES - SUB, LANES), jnp.float32)
    levels = [
        jnp.concatenate(
            [
                jnp.concatenate(
                    [reply_lse[s, :, b * LANES : (b + 1) * LANES], filler], axis=0
                ).T
                for b in range(padded // LANES)
            ],
            axis=0,
        )[:part]
        for s in range(2)
    ]
    attended = []
    for h in range(heads):
        low, high = levels[0][:, h : h + 1], levels[1][:, h : h + 1]
        own = lse_own[h, :part, :]
        top = jnp.maximum(own, jnp.maximum(low, high))
        share_low, share_high = jnp.exp(low - top), jnp.exp(high - top)
        share_own = jnp.exp(own - top)
        total = share_low + share_high + share_own
        summed = (
            share_own * values(mixed_own, h)
            + share_low * reply[0, h].astype(jnp.float32)
            + share_high * reply[1, h].astype(jnp.float32)
        )
        attended.append((summed * (1.0 / total)).astype(jnp.bfloat16))
    updated = nodes[2].astype(jnp.float32) + jnp.dot(
        jnp.concatenate(attended, axis=1), out_w[...], preferred_element_type=jnp.float32
    )
    mean = jnp.sum(updated, axis=1, keepdims=True) / width
    variance = jnp.sum(updated * updated, axis=1, keepdims=True) / width - mean * mean
    result = (updated - mean) * lax.rsqrt(variance + EPSILON)
    for half in range(2):
        normed[half] = (
            result[:, half * side : (half + 1) * side] * gain[half, :1, :]
        ).astype(jnp.bfloat16)

    here = out_ref.at[pl.ds(me * part, part)]
    give = remote(last_copy, normed.at[other], here, partner)
    keep = pltpu.make_async_copy(normed.at[me], here, local_sems.at[0])
    give.start()
    keep.start()
    for group in requests:
        for copy in group:
            copy.wait_send()
    for copy in shared:
        copy.wait_send()
    for sends in replies:
        for copy in sends:
            copy.wait_send()
    keep.wait()
    give.wait()


def shards(
    grid_latent,
    mesh_latent,
    neighbours,
    edge_bias,
    query_weight,
    key_weight,
    value_weight,
    out_weight,
    norm_gain,
):
    band, width = grid_latent.shape
    count, slots = neighbours.shape
    part = count // 2
    cols = width // LANES
    heads = width // HEAD_DIM
    split = heads // 2
    side = width // 2
    per_chunk = LANES // slots
    chunks = part // per_chunk
    padded = -(-part // LANES) * LANES
    me = lax.axis_index("head")
    lat = lax.axis_index("lat")
    size = lax.axis_size("lat")

    flat = neighbours.reshape(2 * chunks, LANES)
    dests = (lax.rem(lat + 1, size), lax.rem(lat + size - 1, size), lat)
    bias = edge_bias.reshape(2, chunks, per_chunk, split, slots).transpose(0, 3, 1, 2, 4)
    bias = bias.reshape(2, split, chunks, LANES)
    orders, biases = [], []
    for dest in dests:
        local = flat - dest * band
        inside = (local >= 0) & (local < band)
        row = jnp.where(inside, local, 0)
        address = (row // SUB) * (SUB * cols) + row % SUB
        orders.append(lax.dynamic_slice_in_dim(address, me * chunks, chunks, 0))
        biases.append(
            jnp.where(inside.reshape(2, 1, chunks, LANES), bias, DEAD)
            .astype(jnp.bfloat16)
            .reshape(2, split * chunks, LANES)
        )
    order_send = jnp.stack(orders[:2])
    bias_send = jnp.stack(biases)
    gain = jnp.broadcast_to(norm_gain.astype(jnp.float32)[None, :], (SUB, side))

    smem = pl.BlockSpec(memory_space=pltpu.SMEM)
    far = pl.BlockSpec(memory_space=pltpu.HBM)
    copies = REQUEST + 2 * REQUEST_COPIES + 2 * (heads + 1) + 1
    bf16, f32 = jnp.bfloat16, jnp.float32
    return pl.pallas_call(
        body,
        name="attend",
        out_shape=jax.ShapeDtypeStruct((count, side), bf16),
        in_specs=[smem] + [far] * 9,
        out_specs=far,
        scratch_shapes=[
            pltpu.VMEM((band * cols, LANES), f32),
            pltpu.VMEM((2, PIECE, width), bf16),
            pltpu.VMEM((GROUP * LANES * cols, LANES), f32),
            pltpu.VMEM((2, width, side), bf16),
            pltpu.VMEM((2, width, side), bf16),
            pltpu.VMEM((2, width, side), bf16),
            pltpu.VMEM((width, width), bf16),
            pltpu.VMEM((2, SUB, side), f32),
            pltpu.VMEM((3, part, width), bf16),
            pltpu.VMEM((2, chunks, LANES), jnp.int32),
            pltpu.SMEM((chunks, LANES), jnp.int32),
            pltpu.SMEM((chunks, LANES), jnp.int32),
            pltpu.VMEM((3, 2, split * chunks, LANES), bf16),
            pltpu.VMEM((heads * chunks, LANES), f32),
            pltpu.VMEM((heads, part, width), f32),
            pltpu.VMEM((heads, part, width), f32),
            pltpu.VMEM((heads, part, width), f32),
            pltpu.VMEM((heads, part, width), f32),
            pltpu.VMEM((heads, padded, LANES), f32),
            pltpu.VMEM((heads, padded, LANES), f32),
            pltpu.VMEM((2, heads, part, HEAD_DIM), bf16),
            pltpu.VMEM((2, SUB, padded), f32),
            pltpu.VMEM((2, heads, part, HEAD_DIM), bf16),
            pltpu.VMEM((2, SUB, padded), f32),
            pltpu.VMEM((2, part, side), bf16),
            pltpu.SemaphoreType.DMA((2,)),
            pltpu.SemaphoreType.DMA((7,)),
            pltpu.SemaphoreType.DMA((2,)),
            pltpu.SemaphoreType.DMA((copies,)),
            pltpu.SemaphoreType.DMA((copies,)),
        ],
        compiler_params=pltpu.CompilerParams(
            collective_id=0, has_side_effects=True, vmem_limit_bytes=56 * 1024 * 1024
        ),
    )(
        orders[2], order_send, bias_send, grid_latent, mesh_latent,
        query_weight, key_weight, value_weight, out_weight, gain,
    )


def solution(mesh):
    in_specs = (
        P("lat", None),
        P("lat", None),
        P("lat", None),
        P("lat", "head"),
        P(None, "head"),
        P(None, "head"),
        P(None, "head"),
        P("head", None),
        P("head"),
    )
    out_specs = P("lat", "head")
    return jax.shard_map(shards, mesh=mesh, in_specs=in_specs, out_specs=out_specs, check_vma=False)
```

```python
import functools

import jax
import jax.numpy as jnp
from jax import lax
from jax.experimental import pallas as pl
from jax.experimental.pallas import tpu as pltpu
from jax.sharding import PartitionSpec as P

HEAD_DIM = 128
LANES = 128
SUB = 8
EPSILON = 1e-05
DEAD = -1e30
PIECE = 1024
HALVES = 2
GROUP = 5
MIX = 10
MESH = pl.DeviceIdType.MESH

SHARED = 0
REQUEST = 6
REQUEST_COPIES = 4
REPLY = REQUEST + 2 * REQUEST_COPIES


def body(
    grid_in, mesh_in, neigh_in, bias_in, query_in, key_in, value_in, out_in, gain_in,
    out_ref,
    wide, stage, picked, rows, query_w, key_w, value_w, out_w, gain_mine, gain_theirs,
    neigh, bias, order_send, bias_send, nodes, order_land, order_own, order_low, order_high,
    bias_land, bias_rows, bias_own, fold, fold_own, scores, weights, mixed, lse,
    mixed_own, lse_own, partial, partial_lse, reply, reply_lse, normed,
    stage_sems, local_sems, order_sems, send_sems, recv_sems,
):
    band, width = grid_in.shape
    part = nodes.shape[1]
    slots, count = neigh.shape
    per_chunk = LANES // slots
    heads = width // HEAD_DIM
    split = heads // 2
    cols = width // LANES
    side = width // 2
    chunks = order_own.shape[0]
    chunk_rows = LANES * cols
    left_rows = heads * SUB
    padded = lse.shape[1]
    piece = part // HALVES
    piece_chunks = chunks // HALVES
    bf16, f32 = jnp.bfloat16, jnp.float32

    lat = lax.axis_index("lat")
    me = lax.axis_index("head")
    size = lax.axis_size("lat")
    other = 1 - me
    partner = (lat, other)
    sides = (
        (lat + 1, lat < size - 1, lat - 1, lat > 0),
        (lat - 1, lat > 0, lat + 1, lat < size - 1),
    )

    def fetch(n):
        return pltpu.make_async_copy(
            grid_in.at[pl.ds(n * PIECE, PIECE)], stage.at[n % 2], stage_sems.at[n % 2]
        )

    mine = [
        pltpu.make_async_copy(src, dst, local_sems.at[n])
        for n, (src, dst) in enumerate((
            (neigh_in, neigh),
            (bias_in, bias),
            (query_in, query_w.at[me]),
            (key_in, key_w.at[me]),
            (value_in, value_w.at[me]),
            (out_in, out_w.at[pl.ds(me * side, side)]),
            (gain_in, gain_mine),
            (mesh_in.at[pl.ds(me * part, part)], nodes.at[2]),
        ))
    ]
    for copy in mine:
        copy.start()
    fetch(0).start()
    fetch(1).start()

    barrier = pltpu.get_barrier_semaphore()

    def signal(device):
        pl.semaphore_signal(barrier, inc=1, device_id=device, device_id_type=MESH)

    signal(partner)
    for target, there, _, _ in sides:
        @pl.when(there)
        def _(target=target):
            signal((target, me))
            signal((target, other))
    pl.semaphore_wait(barrier, 1 + 2 * ((lat + size - 1) // size) + 2 * ((2 * size - 2 - lat) // size))

    def remote(n, src, dst, device):
        return pltpu.make_async_remote_copy(
            src_ref=src, dst_ref=dst, send_sem=send_sems.at[n], recv_sem=recv_sems.at[n],
            device_id=device, device_id_type=MESH,
        )

    def request(s):
        at, target = REQUEST + s * REQUEST_COPIES, sides[s][0]
        order = order_send.at[s, pl.ds(me * chunks, chunks)]
        return (
            remote(at, mesh_in.at[pl.ds(me * part, part)], nodes.at[s], (target, me)),
            remote(at + 1, order, order_land.at[s], (target, me)),
            remote(at + 2, bias_send.at[s, me], bias_land.at[s, me], (target, me)),
            remote(at + 3, bias_send.at[s, other], bias_land.at[s, me], (target, other)),
        )

    def answer(s, half):
        at, target = REPLY + (s * HALVES + half) * 2, sides[s][2]
        return (
            remote(at, partial_lse.at[s, half], reply_lse.at[s, half], (target, me)),
            remote(at + 1, partial.at[s, half], reply.at[s, half], (target, me)),
        )

    shared = [
        remote(SHARED, query_in, query_w.at[me], partner),
        remote(SHARED + 1, key_in, key_w.at[me], partner),
        remote(SHARED + 2, value_in, value_w.at[me], partner),
        remote(SHARED + 3, out_in, out_w.at[pl.ds(me * side, side)], partner),
        remote(SHARED + 4, gain_in, gain_theirs, partner),
        remote(SHARED + 5, bias_send.at[2, other], bias_land.at[2, me], partner),
    ]

    @pl.when(sides[0][1])
    def _():
        request(0)[0].start()

    for copy in shared[:5]:
        copy.start()

    mine[0].wait()
    mine[1].wait()
    index = neigh[...]
    away = jnp.where(index >= 0, index - (lat - 1) * band, 3 * band)
    fields = (
        jnp.right_shift(away, 8).astype(f32).astype(bf16),
        jnp.bitwise_and(away, 255).astype(f32).astype(bf16),
    )

    def iota(shape, axis):
        return lax.broadcasted_iota(jnp.int32, shape, axis)

    def as_mask(value):
        return jnp.where(value, 1.0, 0.0).astype(bf16)

    spread = as_mask(iota((slots, LANES), 0) == iota((slots, LANES), 1) % slots)
    shape = (split * slots, split * LANES)
    spread_bias = as_mask(
        (iota(shape, 0) // slots == iota(shape, 1) // LANES)
        & (iota(shape, 0) % slots == iota(shape, 1) % slots)
    )
    shape = (count, (2 + split) * LANES)
    laid = jnp.concatenate(
        [
            lax.dot_general(value, to, (((0,), (0,)), ((), ())), preferred_element_type=f32)
            for value, to in (*((field, spread) for field in fields), (bias[...], spread_bias))
        ],
        axis=1,
    )
    own_lane = iota(shape, 1) % LANES // slots == iota(shape, 0) % per_chunk
    laid = jnp.where(own_lane, laid, 0.0).astype(bf16)
    shape = (2 * chunks, count)
    gathered = jnp.dot(
        as_mask(iota(shape, 0) == iota(shape, 1) // per_chunk), laid, preferred_element_type=f32
    )
    away = (gathered[:, :LANES] * 256.0 + gathered[:, LANES : 2 * LANES]).astype(jnp.int32)
    for s, step in enumerate((2, 0, 1)):
        local = away - step * band
        inside = (local >= 0) & (local < band)
        row = jnp.where(inside, local, 0)
        order_send[s] = row * cols
        for h in range(split):
            at = (2 + h) * LANES
            masked = jnp.where(inside, gathered[:, at : at + LANES], DEAD).astype(bf16)
            for half in range(2):
                bias_send[s, half, h] = masked[half * chunks : (half + 1) * chunks]

    @pl.when(sides[0][1])
    def _():
        for copy in request(0)[1:]:
            copy.start()

    @pl.when(sides[1][1])
    def _():
        for copy in request(1):
            copy.start()

    shared[5].start()
    keep_bias = pltpu.make_async_copy(bias_send.at[2, me], bias_land.at[2, me], local_sems.at[0])
    keep_bias.start()
    keep_order = pltpu.make_async_copy(
        order_send.at[2, pl.ds(me * chunks, chunks)], order_own, order_sems.at[2]
    )
    keep_order.start()

    pieces = band // PIECE
    for n in range(pieces):
        fetch(n).wait()

        def widen(step, carry, n=n):
            row = pl.multiple_of(step * 32, 32)
            block = stage[n % 2, pl.ds(row, 32), :].astype(f32)
            for t in range(4):
                for c in range(cols):
                    at = (n * PIECE + row + t * SUB) * cols + c
                    wide[pl.ds(at, SUB, stride=cols), :] = block[
                        t * SUB : (t + 1) * SUB, c * LANES : (c + 1) * LANES
                    ]
            return carry

        lax.fori_loop(0, PIECE // 32, widen, 0)
        if n + 2 < pieces:
            fetch(n + 2).start()

    diagonal = iota((SUB, LANES), 1) // slots == iota((SUB, LANES), 0)
    lane = iota((padded, LANES), 1)

    def project(s, fold_ref, bias_ref):
        inputs = nodes[s]
        for half in range(2):
            queries = jnp.dot(inputs, query_w[half], preferred_element_type=f32).astype(bf16)
            for h in range(split):
                span = slice(h * HEAD_DIM, (h + 1) * HEAD_DIM)
                fold_ref[half * split + h] = lax.dot_general(
                    queries[:, span], key_w[half, :, span],
                    (((1,), (1,)), ((), ())), preferred_element_type=f32,
                )
                at = (half * split + h) * chunks
                bias_ref[at : at + chunks, :] = bias_land[s, half, h].astype(f32)

    def gather(order, chunk, u):
        line = order.at[chunk]
        for e in range(LANES):
            at = u * chunk_rows + e * cols
            picked[at : at + cols, :] = wide[pl.ds(line[e], cols), :]

    def block(chunk, size):
        return pl.ds(pl.multiple_of(chunk * size, size), size)

    def score(fold_ref, base, chunk, u):
        found = jnp.concatenate(
            [
                jnp.concatenate(
                    [
                        picked[pl.ds(u * chunk_rows + t * SUB * cols + c, SUB, stride=cols), :]
                        for t in range(LANES // SUB)
                    ],
                    axis=0,
                ).astype(bf16)
                for c in range(cols)
            ],
            axis=1,
        )
        rows[block(chunk, LANES), :] = found
        left = jnp.concatenate(
            [fold_ref[h, block(base + chunk, SUB), :] for h in range(heads)], axis=0
        )
        scores[block(chunk, left_rows), :] = lax.dot_general(
            left.astype(bf16), found, (((1,), (1,)), ((), ())), preferred_element_type=f32
        )

    def soften(bias_ref, lse_ref, base, chunk):
        here = jnp.concatenate(
            [
                jnp.where(diagonal, bias_ref[pl.ds(h * chunks + base + chunk, 1), :], DEAD)
                for h in range(heads)
            ],
            axis=0,
        )
        value = scores[block(chunk, left_rows), :] * HEAD_DIM ** (-0.5) + here
        top = jnp.max(value, axis=1, keepdims=True)
        grown = jnp.exp(value - top)
        total = jnp.sum(grown, axis=1, keepdims=True)
        weights[block(chunk, left_rows), :] = (grown * (1.0 / total)).astype(bf16)
        level = jnp.broadcast_to(top + jnp.log(total), (left_rows, LANES))
        for h in range(heads):
            lse_ref[h, block(chunk, SUB), :] = level[h * SUB : (h + 1) * SUB]

    def mix(mixed_ref, chunk):
        summed = jnp.dot(
            weights[block(chunk, left_rows), :], rows[block(chunk, LANES), :],
            preferred_element_type=f32,
        )
        for h in range(heads):
            mixed_ref[h, block(chunk, SUB), :] = summed[h * SUB : (h + 1) * SUB]

    def run(order, fold_ref, bias_ref, mixed_ref, lse_ref, half):
        base = half * piece_chunks
        for u in range(GROUP):
            gather(order, base + u, u)

        def scoring(n, carry):
            chunk = n * GROUP
            for u in range(GROUP):
                score(fold_ref, base, chunk + u, u)
            for u in range(GROUP):
                gather(order, base + chunk + GROUP + u, u)
            return carry

        lax.fori_loop(0, piece_chunks // GROUP - 1, scoring, 0)
        for u in range(GROUP):
            score(fold_ref, base, piece_chunks - GROUP + u, u)

        def softening(n, carry):
            for u in range(piece_chunks):
                soften(bias_ref, lse_ref, base, n * piece_chunks + u)
            return carry

        lax.fori_loop(0, 1, softening, 0)

        def mixing(n, carry):
            for u in range(MIX):
                mix(mixed_ref, n * MIX + u)
            return carry

        lax.fori_loop(0, piece_chunks // MIX, mixing, 0)

    def values(mixed_ref, h):
        half, inner = h // split, h % split
        return jnp.dot(
            mixed_ref[h].astype(bf16),
            value_w[half, :, inner * HEAD_DIM : (inner + 1) * HEAD_DIM],
            preferred_element_type=f32,
        )

    lse[...] = jnp.zeros(lse.shape, f32)
    for copy in mine[2:]:
        copy.wait()
    for copy in shared:
        copy.wait_recv()
    keep_bias.wait()
    keep_order.wait()

    project(2, fold_own, bias_own)
    run(order_own, fold_own, bias_own, mixed_own.at[0], lse_own.at[0], 0)

    for s, order in enumerate((order_low, order_high)):
        _, sent, _, received = sides[s]

        @pl.when(received)
        def _(s=s, order=order):
            needs = request(s)
            order_copy = pltpu.make_async_copy(order_land.at[s], order, order_sems.at[s])
            for copy in needs:
                copy.wait_recv()
            order_copy.start()
            order_copy.wait()
            project(s, fold, bias_rows)
            for half in range(HALVES):
                run(order, fold, bias_rows, mixed, lse, half)
                level = lse[0]
                for h in range(1, heads):
                    level = jnp.where(lane == h, lse[h], level)
                for b in range(padded // LANES):
                    span = slice(b * LANES, (b + 1) * LANES)
                    partial_lse[s, half, :, span] = level[span].T[:SUB]
                for h in range(heads):
                    partial[s, half, h] = values(mixed, h).astype(bf16)
                for copy in answer(s, half):
                    copy.start()

        @pl.when(jnp.logical_not(sent))
        def _(s=s):
            reply[s] = jnp.zeros(reply.shape[1:], bf16)
            reply_lse[s] = jnp.full(reply_lse.shape[1:], DEAD, f32)

    for half in range(1, HALVES):
        run(order_own, fold_own, bias_own, mixed_own.at[half], lse_own.at[half], half)

    filler = jnp.zeros((LANES - SUB, LANES), f32)
    gains = [
        jnp.where(me == side_of, gain_mine[...], gain_theirs[...]).reshape(1, side).astype(f32)
        for side_of in range(2)
    ]
    give, keep = [], []
    for half in range(HALVES):
        for s in range(2):
            @pl.when(sides[s][1])
            def _(s=s, half=half):
                for copy in answer(s, half):
                    copy.wait_recv()
        levels = [
            jnp.concatenate(
                [
                    jnp.concatenate(
                        [reply_lse[s, half, :, b * LANES : (b + 1) * LANES], filler], axis=0
                    ).T
                    for b in range(padded // LANES)
                ],
                axis=0,
            )[:piece]
            for s in range(2)
        ]
        attended = []
        for h in range(heads):
            low, high = levels[0][:, h : h + 1], levels[1][:, h : h + 1]
            own = lse_own[half, h]
            top = jnp.maximum(own, jnp.maximum(low, high))
            share_low, share_high = jnp.exp(low - top), jnp.exp(high - top)
            share_own = jnp.exp(own - top)
            total = share_low + share_high + share_own
            summed = (
                share_own * values(mixed_own.at[half], h)
                + share_low * reply[0, half, h].astype(f32)
                + share_high * reply[1, half, h].astype(f32)
            )
            attended.append((summed * (1.0 / total)).astype(bf16))
        updated = nodes[2, half * piece : (half + 1) * piece].astype(f32) + jnp.dot(
            jnp.concatenate(attended, axis=1), out_w[...], preferred_element_type=f32
        )
        mean = jnp.sum(updated, axis=1, keepdims=True) / width
        variance = jnp.sum(updated * updated, axis=1, keepdims=True) / width - mean * mean
        result = (updated - mean) * lax.rsqrt(variance + EPSILON)
        for b in range(2):
            normed[half, b] = (result[:, b * side : (b + 1) * side] * gains[b]).astype(bf16)
        here = out_ref.at[pl.ds(me * part + half * piece, piece)]
        at = REPLY + 4 * HALVES + half
        give.append(remote(at, normed.at[half, other], here, partner))
        keep.append(pltpu.make_async_copy(normed.at[half, me], here, local_sems.at[1 + half]))
        give[half].start()
        keep[half].start()

    for copy in shared:
        copy.wait_send()
    for s in range(2):
        @pl.when(sides[s][1])
        def _(s=s):
            for copy in request(s):
                copy.wait_send()

        @pl.when(sides[s][3])
        def _(s=s):
            for half in range(HALVES):
                for copy in answer(s, half):
                    copy.wait_send()
    for copy in keep + give:
        copy.wait()


def shards(
    grid_latent,
    mesh_latent,
    neighbours,
    edge_bias,
    query_weight,
    key_weight,
    value_weight,
    out_weight,
    norm_gain,
):
    band, width = grid_latent.shape
    count, slots = neighbours.shape
    part = count // 2
    cols = width // LANES
    heads = width // HEAD_DIM
    split = heads // 2
    side = width // 2
    chunks = part * slots // LANES
    piece = part // HALVES
    padded = -(-piece // LANES) * LANES
    far = pl.BlockSpec(memory_space=pltpu.HBM)
    copies = REPLY + 5 * HALVES
    bf16, f32, i32 = jnp.bfloat16, jnp.float32, jnp.int32
    return pl.pallas_call(
        body,
        name="attend",
        out_shape=jax.ShapeDtypeStruct((count, side), bf16),
        in_specs=[far] * 9,
        out_specs=far,
        scratch_shapes=[
            pltpu.VMEM((band * cols, LANES), f32),
            pltpu.VMEM((2, PIECE, width), bf16),
            pltpu.VMEM((GROUP * LANES * cols, LANES), f32),
            pltpu.VMEM((piece * slots, width), bf16),
            pltpu.VMEM((2, width, side), bf16),
            pltpu.VMEM((2, width, side), bf16),
            pltpu.VMEM((2, width, side), bf16),
            pltpu.VMEM((width, width), bf16),
            pltpu.VMEM((side,), bf16),
            pltpu.VMEM((side,), bf16),
            pltpu.VMEM((slots, count), i32),
            pltpu.VMEM((split * slots, count), bf16),
            pltpu.VMEM((3, 2 * chunks, LANES), i32),
            pltpu.VMEM((3, 2, split, chunks, LANES), bf16),
            pltpu.VMEM((3, part, width), bf16),
            pltpu.VMEM((2, chunks, LANES), i32),
            pltpu.SMEM((chunks, LANES), i32),
            pltpu.SMEM((chunks, LANES), i32),
            pltpu.SMEM((chunks, LANES), i32),
            pltpu.VMEM((3, 2, split, chunks, LANES), bf16),
            pltpu.VMEM((heads * chunks, LANES), f32),
            pltpu.VMEM((heads * chunks, LANES), f32),
            pltpu.VMEM((heads, part, width), f32),
            pltpu.VMEM((heads, part, width), f32),
            pltpu.VMEM((heads * piece, LANES), f32),
            pltpu.VMEM((heads * piece, LANES), bf16),
            pltpu.VMEM((heads, piece, width), f32),
            pltpu.VMEM((heads, padded, LANES), f32),
            pltpu.VMEM((HALVES, heads, piece, width), f32),
            pltpu.VMEM((HALVES, heads, piece, LANES), f32),
            pltpu.VMEM((2, HALVES, heads, piece, HEAD_DIM), bf16),
            pltpu.VMEM((2, HALVES, SUB, padded), f32),
            pltpu.VMEM((2, HALVES, heads, piece, HEAD_DIM), bf16),
            pltpu.VMEM((2, HALVES, SUB, padded), f32),
            pltpu.VMEM((HALVES, 2, piece, side), bf16),
            pltpu.SemaphoreType.DMA((2,)),
            pltpu.SemaphoreType.DMA((8,)),
            pltpu.SemaphoreType.DMA((3,)),
            pltpu.SemaphoreType.DMA((copies,)),
            pltpu.SemaphoreType.DMA((copies,)),
        ],
        compiler_params=pltpu.CompilerParams(
            collective_id=0, has_side_effects=True, vmem_limit_bytes=56 * 1024 * 1024
        ),
    )(
        grid_latent, mesh_latent, neighbours.T, edge_bias.T,
        query_weight, key_weight, value_weight, out_weight, norm_gain,
    )


def solution(mesh):
    in_specs = (
        P("lat", None),
        P("lat", None),
        P("lat", None),
        P("lat", "head"),
        P(None, "head"),
        P(None, "head"),
        P(None, "head"),
        P("head", None),
        P("head"),
    )
    out_specs = P("lat", "head")
    return jax.shard_map(shards, mesh=mesh, in_specs=in_specs, out_specs=out_specs, check_vma=False)
```

```python
import functools

import jax
import jax.numpy as jnp
from jax import lax
from jax.experimental import pallas as pl
from jax.experimental.pallas import tpu as pltpu
from jax.sharding import PartitionSpec as P

HEAD_DIM = 128
LANES = 128
SUB = 8
EPSILON = 1e-05
DEAD = -1e30
PIECE = 1024
HALVES = 2
GROUP = 5
LEAD = 5
MIX = 10
MESH = pl.DeviceIdType.MESH

SHARED = 0
REQUEST = 6
REQUEST_COPIES = 5
REPLY = REQUEST + 2 * REQUEST_COPIES


def body(
    grid_in, mesh_in, neigh_in, bias_in, query_in, key_in, value_in, out_in, gain_in,
    out_ref,
    wide, stage, picked, rows, query_w, key_w, value_w, out_w, gain_mine, gain_theirs,
    neigh, bias, order_send, bias_send, nodes, order_land, order_own, order_low, order_high,
    bias_land, bias_rows, bias_own, fold, fold_own, scores, weights, mixed, lse,
    mixed_own, lse_own, partial, partial_lse, reply, reply_lse, normed,
    stage_sems, local_sems, order_sems, send_sems, recv_sems,
):
    band, width = grid_in.shape
    part = nodes.shape[1]
    slots, count = neigh.shape
    per_chunk = LANES // slots
    heads = width // HEAD_DIM
    split = heads // 2
    cols = width // LANES
    side = width // 2
    chunks = order_own.shape[0]
    chunk_rows = LANES * cols
    left_rows = heads * SUB
    padded = lse.shape[1]
    piece = part // HALVES
    piece_chunks = chunks // HALVES
    bf16, f32 = jnp.bfloat16, jnp.float32

    lat = lax.axis_index("lat")
    me = lax.axis_index("head")
    size = lax.axis_size("lat")
    other = 1 - me
    partner = (lat, other)
    sides = (
        (lat + 1, lat < size - 1, lat - 1, lat > 0),
        (lat - 1, lat > 0, lat + 1, lat < size - 1),
    )

    def fetch(n):
        return pltpu.make_async_copy(
            grid_in.at[pl.ds(n * PIECE, PIECE)], stage.at[n % 2], stage_sems.at[n % 2]
        )

    mine = [
        pltpu.make_async_copy(src, dst, local_sems.at[n])
        for n, (src, dst) in enumerate((
            (neigh_in, neigh),
            (bias_in, bias),
            (query_in, query_w.at[me]),
            (key_in, key_w.at[me]),
            (value_in, value_w.at[me]),
            (out_in, out_w.at[pl.ds(me * side, side)]),
            (gain_in, gain_mine),
            (mesh_in.at[pl.ds(me * part, part)], nodes.at[2]),
        ))
    ]
    for copy in mine:
        copy.start()
    fetch(0).start()
    fetch(1).start()

    barrier = pltpu.get_barrier_semaphore()

    def signal(device):
        pl.semaphore_signal(barrier, inc=1, device_id=device, device_id_type=MESH)

    signal(partner)
    for target, there, _, _ in sides:
        @pl.when(there)
        def _(target=target):
            signal((target, me))
            signal((target, other))
    pl.semaphore_wait(barrier, 1 + 2 * ((lat + size - 1) // size) + 2 * ((2 * size - 2 - lat) // size))

    def remote(n, src, dst, device):
        return pltpu.make_async_remote_copy(
            src_ref=src, dst_ref=dst, send_sem=send_sems.at[n], recv_sem=recv_sems.at[n],
            device_id=device, device_id_type=MESH,
        )

    def request(s):
        at, target = REQUEST + s * REQUEST_COPIES, sides[s][0]
        order = order_send.at[s, pl.ds(me * chunks, chunks)]
        lead, rest = pl.ds(0, part // LEAD), pl.ds(part // LEAD, part - part // LEAD)
        mesh_rows = mesh_in.at[pl.ds(me * part, part)]
        return (
            remote(at, mesh_rows.at[lead], nodes.at[s, lead], (target, me)),
            remote(at + 1, order, order_land.at[s], (target, me)),
            remote(at + 2, bias_send.at[s, me], bias_land.at[s, me], (target, me)),
            remote(at + 3, bias_send.at[s, other], bias_land.at[s, me], (target, other)),
            remote(at + 4, mesh_rows.at[rest], nodes.at[s, rest], (target, me)),
        )

    def answer(s, half):
        at, target = REPLY + (s * HALVES + half) * 2, sides[s][2]
        return (
            remote(at, partial_lse.at[s, half], reply_lse.at[s, half], (target, me)),
            remote(at + 1, partial.at[s, half], reply.at[s, half], (target, me)),
        )

    shared = [
        remote(SHARED, query_in, query_w.at[me], partner),
        remote(SHARED + 1, key_in, key_w.at[me], partner),
        remote(SHARED + 2, value_in, value_w.at[me], partner),
        remote(SHARED + 3, out_in, out_w.at[pl.ds(me * side, side)], partner),
        remote(SHARED + 4, gain_in, gain_theirs, partner),
        remote(SHARED + 5, bias_send.at[2, other], bias_land.at[2, me], partner),
    ]

    @pl.when(sides[0][1])
    def _():
        request(0)[0].start()

    for copy in shared[:5]:
        copy.start()

    mine[0].wait()
    mine[1].wait()
    index = neigh[...]
    away = jnp.where(index >= 0, index - (lat - 1) * band, 3 * band)
    fields = (
        jnp.right_shift(away, 8).astype(f32).astype(bf16),
        jnp.bitwise_and(away, 255).astype(f32).astype(bf16),
    )

    def iota(shape, axis):
        return lax.broadcasted_iota(jnp.int32, shape, axis)

    def as_mask(value):
        return jnp.where(value, 1.0, 0.0).astype(bf16)

    spread = as_mask(iota((slots, LANES), 0) == iota((slots, LANES), 1) % slots)
    shape = (split * slots, split * LANES)
    spread_bias = as_mask(
        (iota(shape, 0) // slots == iota(shape, 1) // LANES)
        & (iota(shape, 0) % slots == iota(shape, 1) % slots)
    )
    shape = (count, (2 + split) * LANES)
    laid = jnp.concatenate(
        [
            lax.dot_general(value, to, (((0,), (0,)), ((), ())), preferred_element_type=f32)
            for value, to in (*((field, spread) for field in fields), (bias[...], spread_bias))
        ],
        axis=1,
    )
    own_lane = iota(shape, 1) % LANES // slots == iota(shape, 0) % per_chunk
    laid = jnp.where(own_lane, laid, 0.0).astype(bf16)
    shape = (2 * chunks, count)
    gathered = jnp.dot(
        as_mask(iota(shape, 0) == iota(shape, 1) // per_chunk), laid, preferred_element_type=f32
    )
    away = (gathered[:, :LANES] * 256.0 + gathered[:, LANES : 2 * LANES]).astype(jnp.int32)
    for s, step in enumerate((2, 0, 1)):
        local = away - step * band
        inside = (local >= 0) & (local < band)
        row = jnp.where(inside, local, 0)
        order_send[s] = row * cols
        for h in range(split):
            at = (2 + h) * LANES
            masked = jnp.where(inside, gathered[:, at : at + LANES], DEAD).astype(bf16)
            for half in range(2):
                bias_send[s, half, h] = masked[half * chunks : (half + 1) * chunks]

    @pl.when(sides[0][1])
    def _():
        for copy in request(0)[1:]:
            copy.start()

    @pl.when(sides[1][1])
    def _():
        for copy in request(1)[1:4]:
            copy.start()

    shared[5].start()
    keep_bias = pltpu.make_async_copy(bias_send.at[2, me], bias_land.at[2, me], local_sems.at[0])
    keep_bias.start()
    keep_order = pltpu.make_async_copy(
        order_send.at[2, pl.ds(me * chunks, chunks)], order_own, order_sems.at[2]
    )
    keep_order.start()

    diagonal = iota((SUB, LANES), 1) // slots == iota((SUB, LANES), 0)
    lane = iota((padded, LANES), 1)

    def project(s, fold_ref, bias_ref):
        inputs = nodes[s]
        for half in range(2):
            queries = jnp.dot(inputs, query_w[half], preferred_element_type=f32).astype(bf16)
            for h in range(split):
                span = slice(h * HEAD_DIM, (h + 1) * HEAD_DIM)
                fold_ref[half * split + h] = lax.dot_general(
                    queries[:, span], key_w[half, :, span],
                    (((1,), (1,)), ((), ())), preferred_element_type=f32,
                )
                at = (half * split + h) * chunks
                bias_ref[at : at + chunks, :] = bias_land[s, half, h].astype(f32)

    def gather(order, chunk, u):
        line = order.at[chunk]
        for e in range(LANES):
            at = u * chunk_rows + e * cols
            picked[at : at + cols, :] = wide[pl.ds(line[e], cols), :]

    def block(chunk, size):
        return pl.ds(pl.multiple_of(chunk * size, size), size)

    def score(fold_ref, base, chunk, u):
        found = jnp.concatenate(
            [
                jnp.concatenate(
                    [
                        picked[pl.ds(u * chunk_rows + t * SUB * cols + c, SUB, stride=cols), :]
                        for t in range(LANES // SUB)
                    ],
                    axis=0,
                ).astype(bf16)
                for c in range(cols)
            ],
            axis=1,
        )
        rows[block(chunk, LANES), :] = found
        left = jnp.concatenate(
            [fold_ref[h, block(base + chunk, SUB), :] for h in range(heads)], axis=0
        )
        scores[block(chunk, left_rows), :] = lax.dot_general(
            left.astype(bf16), found, (((1,), (1,)), ((), ())), preferred_element_type=f32
        )

    def soften(bias_ref, lse_ref, base, chunk):
        here = jnp.concatenate(
            [
                jnp.where(diagonal, bias_ref[pl.ds(h * chunks + base + chunk, 1), :], DEAD)
                for h in range(heads)
            ],
            axis=0,
        )
        value = scores[block(chunk, left_rows), :] * HEAD_DIM ** (-0.5) + here
        top = jnp.max(value, axis=1, keepdims=True)
        grown = jnp.exp(value - top)
        total = jnp.sum(grown, axis=1, keepdims=True)
        weights[block(chunk, left_rows), :] = (grown * (1.0 / total)).astype(bf16)
        level = jnp.broadcast_to(top + jnp.log(total), (left_rows, LANES))
        for h in range(heads):
            lse_ref[h, block(chunk, SUB), :] = level[h * SUB : (h + 1) * SUB]

    def mix(mixed_ref, chunk):
        summed = jnp.dot(
            weights[block(chunk, left_rows), :], rows[block(chunk, LANES), :],
            preferred_element_type=f32,
        )
        for h in range(heads):
            mixed_ref[h, block(chunk, SUB), :] = summed[h * SUB : (h + 1) * SUB]

    def run(order, fold_ref, bias_ref, mixed_ref, lse_ref, half, then=None):
        base = half * piece_chunks
        for u in range(GROUP):
            gather(order, base + u, u)

        def scoring(n, carry):
            chunk = n * GROUP
            for u in range(GROUP):
                score(fold_ref, base, chunk + u, u)
            for u in range(GROUP):
                gather(order, base + chunk + GROUP + u, u)
            return carry

        lax.fori_loop(0, piece_chunks // GROUP - 1, scoring, 0)
        for u in range(GROUP):
            score(fold_ref, base, piece_chunks - GROUP + u, u)
        if then is not None:
            then()

        def softening(n, carry):
            for u in range(piece_chunks):
                soften(bias_ref, lse_ref, base, n * piece_chunks + u)
            return carry

        lax.fori_loop(0, 1, softening, 0)

        def mixing(n, carry):
            for u in range(MIX):
                mix(mixed_ref, n * MIX + u)
            return carry

        lax.fori_loop(0, piece_chunks // MIX, mixing, 0)

    def values(mixed_ref, h):
        half, inner = h // split, h % split
        return jnp.dot(
            mixed_ref[h].astype(bf16),
            value_w[half, :, inner * HEAD_DIM : (inner + 1) * HEAD_DIM],
            preferred_element_type=f32,
        )

    def address(s):
        order = (order_low, order_high)[s]
        return pltpu.make_async_copy(order_land.at[s], order, order_sems.at[s])

    lse[...] = jnp.zeros(lse.shape, f32)
    pieces = band // PIECE
    for n in range(pieces):
        fetch(n).wait()

        def widen(step, carry, n=n):
            row = pl.multiple_of(step * 32, 32)
            block = stage[n % 2, pl.ds(row, 32), :].astype(f32)
            for t in range(4):
                for c in range(cols):
                    at = (n * PIECE + row + t * SUB) * cols + c
                    wide[pl.ds(at, SUB, stride=cols), :] = block[
                        t * SUB : (t + 1) * SUB, c * LANES : (c + 1) * LANES
                    ]
            return carry

        lax.fori_loop(0, PIECE // 32, widen, 0)
        if n + 2 < pieces:
            fetch(n + 2).start()
        if n == pieces // 2:
            for copy in mine[2:]:
                copy.wait()
            for copy in shared:
                copy.wait_recv()
            keep_bias.wait()
            project(2, fold_own, bias_own)

    @pl.when(sides[0][3])
    def _():
        request(0)[1].wait_recv()
        address(0).start()

    keep_order.wait()

    def send_down():
        @pl.when(sides[1][1])
        def _():
            request(1)[0].start()
            request(1)[4].start()

    run(order_own, fold_own, bias_own, mixed_own.at[0], lse_own.at[0], 0, send_down)

    def arrive(s):
        address(s).wait()
        for n in (2, 3, 0, 4):
            request(s)[n].wait_recv()

    @pl.when(sides[0][3])
    def _():
        arrive(0)

    @pl.when(sides[1][3])
    def _():
        request(1)[1].wait_recv()
        address(1).start()

    for s, order in enumerate((order_low, order_high)):
        _, sent, _, received = sides[s]

        @pl.when(received)
        def _(s=s, order=order):
            if s:
                arrive(s)
            project(s, fold, bias_rows)
            for half in range(HALVES):
                run(order, fold, bias_rows, mixed, lse, half)
                level = lse[0]
                for h in range(1, heads):
                    level = jnp.where(lane == h, lse[h], level)
                for b in range(padded // LANES):
                    span = slice(b * LANES, (b + 1) * LANES)
                    partial_lse[s, half, :, span] = level[span].T[:SUB]
                for h in range(heads):
                    partial[s, half, h] = values(mixed, h).astype(bf16)
                for copy in answer(s, half):
                    copy.start()

        @pl.when(jnp.logical_not(sent))
        def _(s=s):
            reply[s] = jnp.zeros(reply.shape[1:], bf16)
            reply_lse[s] = jnp.full(reply_lse.shape[1:], DEAD, f32)

    for half in range(1, HALVES):
        run(order_own, fold_own, bias_own, mixed_own.at[half], lse_own.at[half], half)

    filler = jnp.zeros((LANES - SUB, LANES), f32)
    gains = [
        jnp.where(me == side_of, gain_mine[...], gain_theirs[...]).reshape(1, side).astype(f32)
        for side_of in range(2)
    ]
    give, keep = [], []
    for half in range(HALVES):
        for s in range(2):
            @pl.when(sides[s][1])
            def _(s=s, half=half):
                for copy in answer(s, half):
                    copy.wait_recv()
        levels = [
            jnp.concatenate(
                [
                    jnp.concatenate(
                        [reply_lse[s, half, :, b * LANES : (b + 1) * LANES], filler], axis=0
                    ).T
                    for b in range(padded // LANES)
                ],
                axis=0,
            )[:piece]
            for s in range(2)
        ]
        attended = []
        for h in range(heads):
            low, high = levels[0][:, h : h + 1], levels[1][:, h : h + 1]
            own = lse_own[half, h]
            top = jnp.maximum(own, jnp.maximum(low, high))
            share_low, share_high = jnp.exp(low - top), jnp.exp(high - top)
            share_own = jnp.exp(own - top)
            total = share_low + share_high + share_own
            summed = (
                share_own * values(mixed_own.at[half], h)
                + share_low * reply[0, half, h].astype(f32)
                + share_high * reply[1, half, h].astype(f32)
            )
            attended.append((summed * (1.0 / total)).astype(bf16))
        updated = nodes[2, half * piece : (half + 1) * piece].astype(f32) + jnp.dot(
            jnp.concatenate(attended, axis=1), out_w[...], preferred_element_type=f32
        )
        mean = jnp.sum(updated, axis=1, keepdims=True) / width
        variance = jnp.sum(updated * updated, axis=1, keepdims=True) / width - mean * mean
        result = (updated - mean) * lax.rsqrt(variance + EPSILON)
        for b in range(2):
            normed[half, b] = (result[:, b * side : (b + 1) * side] * gains[b]).astype(bf16)
        here = out_ref.at[pl.ds(me * part + half * piece, piece)]
        at = REPLY + 4 * HALVES + half
        give.append(remote(at, normed.at[half, other], here, partner))
        keep.append(pltpu.make_async_copy(normed.at[half, me], here, local_sems.at[1 + half]))
        give[half].start()
        keep[half].start()

    for copy in shared:
        copy.wait_send()
    for s in range(2):
        @pl.when(sides[s][1])
        def _(s=s):
            for copy in request(s):
                copy.wait_send()

        @pl.when(sides[s][3])
        def _(s=s):
            for half in range(HALVES):
                for copy in answer(s, half):
                    copy.wait_send()
    for copy in keep + give:
        copy.wait()


def shards(
    grid_latent,
    mesh_latent,
    neighbours,
    edge_bias,
    query_weight,
    key_weight,
    value_weight,
    out_weight,
    norm_gain,
):
    band, width = grid_latent.shape
    count, slots = neighbours.shape
    part = count // 2
    cols = width // LANES
    heads = width // HEAD_DIM
    split = heads // 2
    side = width // 2
    chunks = part * slots // LANES
    piece = part // HALVES
    padded = -(-piece // LANES) * LANES
    far = pl.BlockSpec(memory_space=pltpu.HBM)
    copies = REPLY + 5 * HALVES
    bf16, f32, i32 = jnp.bfloat16, jnp.float32, jnp.int32
    return pl.pallas_call(
        body,
        name="attend",
        out_shape=jax.ShapeDtypeStruct((count, side), bf16),
        in_specs=[far] * 9,
        out_specs=far,
        scratch_shapes=[
            pltpu.VMEM((band * cols, LANES), f32),
            pltpu.VMEM((2, PIECE, width), bf16),
            pltpu.VMEM((GROUP * LANES * cols, LANES), f32),
            pltpu.VMEM((piece * slots, width), bf16),
            pltpu.VMEM((2, width, side), bf16),
            pltpu.VMEM((2, width, side), bf16),
            pltpu.VMEM((2, width, side), bf16),
            pltpu.VMEM((width, width), bf16),
            pltpu.VMEM((side,), bf16),
            pltpu.VMEM((side,), bf16),
            pltpu.VMEM((slots, count), i32),
            pltpu.VMEM((split * slots, count), bf16),
            pltpu.VMEM((3, 2 * chunks, LANES), i32),
            pltpu.VMEM((3, 2, split, chunks, LANES), bf16),
            pltpu.VMEM((3, part, width), bf16),
            pltpu.VMEM((2, chunks, LANES), i32),
            pltpu.SMEM((chunks, LANES), i32),
            pltpu.SMEM((chunks, LANES), i32),
            pltpu.SMEM((chunks, LANES), i32),
            pltpu.VMEM((3, 2, split, chunks, LANES), bf16),
            pltpu.VMEM((heads * chunks, LANES), f32),
            pltpu.VMEM((heads * chunks, LANES), f32),
            pltpu.VMEM((heads, part, width), f32),
            pltpu.VMEM((heads, part, width), f32),
            pltpu.VMEM((heads * piece, LANES), f32),
            pltpu.VMEM((heads * piece, LANES), bf16),
            pltpu.VMEM((heads, piece, width), f32),
            pltpu.VMEM((heads, padded, LANES), f32),
            pltpu.VMEM((HALVES, heads, piece, width), f32),
            pltpu.VMEM((HALVES, heads, piece, LANES), f32),
            pltpu.VMEM((2, HALVES, heads, piece, HEAD_DIM), bf16),
            pltpu.VMEM((2, HALVES, SUB, padded), f32),
            pltpu.VMEM((2, HALVES, heads, piece, HEAD_DIM), bf16),
            pltpu.VMEM((2, HALVES, SUB, padded), f32),
            pltpu.VMEM((HALVES, 2, piece, side), bf16),
            pltpu.SemaphoreType.DMA((2,)),
            pltpu.SemaphoreType.DMA((8,)),
            pltpu.SemaphoreType.DMA((3,)),
            pltpu.SemaphoreType.DMA((copies,)),
            pltpu.SemaphoreType.DMA((copies,)),
        ],
        compiler_params=pltpu.CompilerParams(
            collective_id=0, has_side_effects=True, vmem_limit_bytes=56 * 1024 * 1024
        ),
    )(
        grid_latent, mesh_latent, neighbours.T, edge_bias.T,
        query_weight, key_weight, value_weight, out_weight, norm_gain,
    )


def solution(mesh):
    in_specs = (
        P("lat", None),
        P("lat", None),
        P("lat", None),
        P("lat", "head"),
        P(None, "head"),
        P(None, "head"),
        P(None, "head"),
        P("head", None),
        P("head"),
    )
    out_specs = P("lat", "head")
    return jax.shard_map(shards, mesh=mesh, in_specs=in_specs, out_specs=out_specs, check_vma=False)
```

```python
import functools

import jax
import jax.numpy as jnp
from jax import lax
from jax.experimental import pallas as pl
from jax.experimental.pallas import tpu as pltpu
from jax.sharding import PartitionSpec as P

HEAD_DIM = 128
LANES = 128
SUB = 8
EPSILON = 1e-05
DEAD = -1e30
PIECE = 1024
HALVES = 2
GROUP = 5
LEAD = 5
MIX = 10
MESH = pl.DeviceIdType.MESH

SHARED = 0
REQUEST = 6
REQUEST_COPIES = 5
REPLY = REQUEST + 2 * REQUEST_COPIES


def body(
    grid_in, mesh_in, neigh_in, bias_in, query_in, key_in, value_in, out_in, gain_in,
    out_ref,
    wide, stage, picked, rows, query_w, key_w, value_w, out_w, gain_mine, gain_theirs,
    neigh, bias, order_send, bias_send, nodes, order_land, order_own, order_low, order_high,
    bias_land, bias_rows, bias_own, fold, fold_own, scores, weights, mixed, lse,
    mixed_own, lse_own, partial, partial_lse, reply, reply_lse, normed, landed,
    stage_sems, local_sems, order_sems, send_sems, recv_sems,
):
    band, width = grid_in.shape
    part = nodes.shape[1]
    slots, count = neigh.shape
    per_chunk = LANES // slots
    heads = width // HEAD_DIM
    split = heads // 2
    cols = width // LANES
    side = width // 2
    chunks = order_own.shape[0]
    chunk_rows = LANES * cols
    left_rows = heads * SUB
    padded = lse.shape[1]
    piece = part // HALVES
    piece_chunks = chunks // HALVES
    bf16, f32 = jnp.bfloat16, jnp.float32

    lat = lax.axis_index("lat")
    me = lax.axis_index("head")
    size = lax.axis_size("lat")
    other = 1 - me
    partner = (lat, other)
    sides = (
        (lat + 1, lat < size - 1, lat - 1, lat > 0),
        (lat - 1, lat > 0, lat + 1, lat < size - 1),
    )

    def fetch(n):
        return pltpu.make_async_copy(
            grid_in.at[pl.ds(n * PIECE, PIECE)], stage.at[n % 2], stage_sems.at[n % 2]
        )

    mine = [
        pltpu.make_async_copy(src, dst, local_sems.at[n])
        for n, (src, dst) in enumerate((
            (neigh_in, neigh),
            (bias_in, bias),
            (query_in, query_w.at[me]),
            (key_in, key_w.at[me]),
            (value_in, value_w.at[me]),
            (out_in, out_w.at[pl.ds(me * side, side)]),
            (gain_in, gain_mine),
            (mesh_in.at[pl.ds(me * part, part)], nodes.at[2]),
        ))
    ]
    for copy in mine:
        copy.start()
    fetch(0).start()
    fetch(1).start()

    barrier = pltpu.get_barrier_semaphore()

    def signal(device):
        pl.semaphore_signal(barrier, inc=1, device_id=device, device_id_type=MESH)

    signal(partner)
    for target, there, _, _ in sides:
        @pl.when(there)
        def _(target=target):
            signal((target, me))
            signal((target, other))
    pl.semaphore_wait(barrier, 1 + 2 * ((lat + size - 1) // size) + 2 * ((2 * size - 2 - lat) // size))

    def remote(n, src, dst, device):
        return pltpu.make_async_remote_copy(
            src_ref=src, dst_ref=dst, send_sem=send_sems.at[n], recv_sem=recv_sems.at[n],
            device_id=device, device_id_type=MESH,
        )

    def request(s):
        at, target = REQUEST + s * REQUEST_COPIES, sides[s][0]
        order = order_send.at[s, pl.ds(me * chunks, chunks)]
        lead, rest = pl.ds(0, part // LEAD), pl.ds(part // LEAD, part - part // LEAD)
        mesh_rows = mesh_in.at[pl.ds(me * part, part)]
        return (
            remote(at, mesh_rows.at[lead], nodes.at[s, lead], (target, me)),
            remote(at + 1, order, order_land.at[s], (target, me)),
            remote(at + 2, bias_send.at[s, me], bias_land.at[s, me], (target, me)),
            remote(at + 3, bias_send.at[s, other], bias_land.at[s, me], (target, other)),
            remote(at + 4, mesh_rows.at[rest], nodes.at[s, rest], (target, me)),
        )

    def answer(s, half):
        at, target = REPLY + (s * HALVES + half) * 2, sides[s][2]
        return (
            remote(at, partial_lse.at[s, half], reply_lse.at[s, half], (target, me)),
            remote(at + 1, partial.at[s, half], reply.at[s, half], (target, me)),
        )

    shared = [
        remote(SHARED, query_in, query_w.at[me], partner),
        remote(SHARED + 1, key_in, key_w.at[me], partner),
        remote(SHARED + 2, value_in, value_w.at[me], partner),
        remote(SHARED + 3, out_in, out_w.at[pl.ds(me * side, side)], partner),
        remote(SHARED + 4, gain_in, gain_theirs, partner),
        remote(SHARED + 5, bias_send.at[2, other], bias_land.at[2, me], partner),
    ]

    @pl.when(sides[0][1])
    def _():
        request(0)[0].start()

    for copy in shared[:5]:
        copy.start()

    mine[0].wait()
    mine[1].wait()
    index = neigh[...]
    away = jnp.where(index >= 0, index - (lat - 1) * band, 3 * band)
    fields = (
        jnp.right_shift(away, 8).astype(f32).astype(bf16),
        jnp.bitwise_and(away, 255).astype(f32).astype(bf16),
    )

    def iota(shape, axis):
        return lax.broadcasted_iota(jnp.int32, shape, axis)

    def as_mask(value):
        return jnp.where(value, 1.0, 0.0).astype(bf16)

    spread = as_mask(iota((slots, LANES), 0) == iota((slots, LANES), 1) % slots)
    shape = (split * slots, split * LANES)
    spread_bias = as_mask(
        (iota(shape, 0) // slots == iota(shape, 1) // LANES)
        & (iota(shape, 0) % slots == iota(shape, 1) % slots)
    )
    shape = (count, (2 + split) * LANES)
    laid = jnp.concatenate(
        [
            lax.dot_general(value, to, (((0,), (0,)), ((), ())), preferred_element_type=f32)
            for value, to in (*((field, spread) for field in fields), (bias[...], spread_bias))
        ],
        axis=1,
    )
    own_lane = iota(shape, 1) % LANES // slots == iota(shape, 0) % per_chunk
    laid = jnp.where(own_lane, laid, 0.0).astype(bf16)
    shape = (2 * chunks, count)
    gathered = jnp.dot(
        as_mask(iota(shape, 0) == iota(shape, 1) // per_chunk), laid, preferred_element_type=f32
    )
    away = (gathered[:, :LANES] * 256.0 + gathered[:, LANES : 2 * LANES]).astype(jnp.int32)
    for s, step in enumerate((2, 0, 1)):
        local = away - step * band
        inside = (local >= 0) & (local < band)
        row = jnp.where(inside, local, 0)
        order_send[s] = row * cols
        for h in range(split):
            at = (2 + h) * LANES
            masked = jnp.where(inside, gathered[:, at : at + LANES], DEAD).astype(bf16)
            for half in range(2):
                bias_send[s, half, h] = masked[half * chunks : (half + 1) * chunks]

    @pl.when(sides[0][1])
    def _():
        for copy in request(0)[1:]:
            copy.start()

    @pl.when(sides[1][1])
    def _():
        for copy in request(1)[1:4]:
            copy.start()

    shared[5].start()
    keep_bias = pltpu.make_async_copy(bias_send.at[2, me], bias_land.at[2, me], local_sems.at[0])
    keep_bias.start()
    keep_order = pltpu.make_async_copy(
        order_send.at[2, pl.ds(me * chunks, chunks)], order_own, order_sems.at[2]
    )
    keep_order.start()

    diagonal = iota((SUB, LANES), 1) // slots == iota((SUB, LANES), 0)
    lane = iota((padded, LANES), 1)

    def project(s, fold_ref, bias_ref):
        inputs = nodes[s]
        for half in range(2):
            queries = jnp.dot(inputs, query_w[half], preferred_element_type=f32).astype(bf16)
            for h in range(split):
                span = slice(h * HEAD_DIM, (h + 1) * HEAD_DIM)
                fold_ref[half * split + h] = lax.dot_general(
                    queries[:, span], key_w[half, :, span],
                    (((1,), (1,)), ((), ())), preferred_element_type=f32,
                )
                at = (half * split + h) * chunks
                bias_ref[at : at + chunks, :] = bias_land[s, half, h].astype(f32)

    def gather(order, chunk, u):
        line = order.at[chunk]
        for e in range(LANES):
            at = u * chunk_rows + e * cols
            picked[at : at + cols, :] = wide[pl.ds(line[e], cols), :]

    def block(chunk, size):
        return pl.ds(pl.multiple_of(chunk * size, size), size)

    def score(fold_ref, base, chunk, u):
        found = jnp.concatenate(
            [
                jnp.concatenate(
                    [
                        picked[pl.ds(u * chunk_rows + t * SUB * cols + c, SUB, stride=cols), :]
                        for t in range(LANES // SUB)
                    ],
                    axis=0,
                ).astype(bf16)
                for c in range(cols)
            ],
            axis=1,
        )
        rows[block(chunk, LANES), :] = found
        left = jnp.concatenate(
            [fold_ref[h, block(base + chunk, SUB), :] for h in range(heads)], axis=0
        )
        scores[block(chunk, left_rows), :] = lax.dot_general(
            left.astype(bf16), found, (((1,), (1,)), ((), ())), preferred_element_type=f32
        )

    def soften(bias_ref, lse_ref, base, chunk):
        here = jnp.concatenate(
            [
                jnp.where(diagonal, bias_ref[pl.ds(h * chunks + base + chunk, 1), :], DEAD)
                for h in range(heads)
            ],
            axis=0,
        )
        value = scores[block(chunk, left_rows), :] * HEAD_DIM ** (-0.5) + here
        top = jnp.max(value, axis=1, keepdims=True)
        grown = jnp.exp(value - top)
        total = jnp.sum(grown, axis=1, keepdims=True)
        weights[block(chunk, left_rows), :] = (grown * (1.0 / total)).astype(bf16)
        level = jnp.broadcast_to(top + jnp.log(total), (left_rows, LANES))
        for h in range(heads):
            lse_ref[h, block(chunk, SUB), :] = level[h * SUB : (h + 1) * SUB]

    def mix(mixed_ref, chunk):
        summed = jnp.dot(
            weights[block(chunk, left_rows), :], rows[block(chunk, LANES), :],
            preferred_element_type=f32,
        )
        for h in range(heads):
            mixed_ref[h, block(chunk, SUB), :] = summed[h * SUB : (h + 1) * SUB]

    def run(order, fold_ref, bias_ref, mixed_ref, lse_ref, half, then=None):
        base = half * piece_chunks
        for u in range(GROUP):
            gather(order, base + u, u)

        def scoring(n, carry):
            chunk = n * GROUP
            for u in range(GROUP):
                score(fold_ref, base, chunk + u, u)
            for u in range(GROUP):
                gather(order, base + chunk + GROUP + u, u)
            return carry

        lax.fori_loop(0, piece_chunks // GROUP - 1, scoring, 0)
        for u in range(GROUP):
            score(fold_ref, base, piece_chunks - GROUP + u, u)
        if then is not None:
            then()

        def softening(n, carry):
            for u in range(piece_chunks):
                soften(bias_ref, lse_ref, base, n * piece_chunks + u)
            return carry

        lax.fori_loop(0, 1, softening, 0)

        def mixing(n, carry):
            for u in range(MIX):
                mix(mixed_ref, n * MIX + u)
            return carry

        lax.fori_loop(0, piece_chunks // MIX, mixing, 0)

    def values(mixed_ref, h):
        half, inner = h // split, h % split
        return jnp.dot(
            mixed_ref[h].astype(bf16),
            value_w[half, :, inner * HEAD_DIM : (inner + 1) * HEAD_DIM],
            preferred_element_type=f32,
        )

    def address(s):
        order = (order_low, order_high)[s]
        return pltpu.make_async_copy(order_land.at[s], order, order_sems.at[s])

    lse[...] = jnp.zeros(lse.shape, f32)
    pieces = band // PIECE
    for n in range(pieces):
        fetch(n).wait()

        def widen(step, carry, n=n):
            row = pl.multiple_of(step * 32, 32)
            block = stage[n % 2, pl.ds(row, 32), :].astype(f32)
            for t in range(4):
                for c in range(cols):
                    at = (n * PIECE + row + t * SUB) * cols + c
                    wide[pl.ds(at, SUB, stride=cols), :] = block[
                        t * SUB : (t + 1) * SUB, c * LANES : (c + 1) * LANES
                    ]
            return carry

        lax.fori_loop(0, PIECE // 32, widen, 0)
        if n + 2 < pieces:
            fetch(n + 2).start()
        if n == pieces // 2:
            for copy in mine[2:]:
                copy.wait()
            for copy in shared:
                copy.wait_recv()
            keep_bias.wait()
            project(2, fold_own, bias_own)

    @pl.when(sides[0][3])
    def _():
        request(0)[1].wait_recv()
        address(0).start()

    keep_order.wait()

    def send_down():
        @pl.when(sides[1][1])
        def _():
            request(1)[0].start()
            request(1)[4].start()

    run(order_own, fold_own, bias_own, mixed_own.at[0], lse_own.at[0], 0, send_down)

    def arrive(s):
        address(s).wait()
        for n in (2, 3, 0, 4):
            request(s)[n].wait_recv()

    @pl.when(sides[0][3])
    def _():
        arrive(0)

    @pl.when(sides[1][3])
    def _():
        request(1)[1].wait_recv()
        address(1).start()

    for s, order in enumerate((order_low, order_high)):
        _, sent, _, received = sides[s]

        @pl.when(received)
        def _(s=s, order=order):
            if s:
                arrive(s)
            project(s, fold, bias_rows)
            for half in range(HALVES):
                run(order, fold, bias_rows, mixed, lse, half)
                level = lse[0]
                for h in range(1, heads):
                    level = jnp.where(lane == h, lse[h], level)
                for b in range(padded // LANES):
                    span = slice(b * LANES, (b + 1) * LANES)
                    partial_lse[s, half, :, span] = level[span].T[:SUB]
                for h in range(heads):
                    partial[s, half, h] = values(mixed, h).astype(bf16)
                for copy in answer(s, half):
                    copy.start()

        @pl.when(jnp.logical_not(sent))
        def _(s=s):
            reply[s] = jnp.zeros(reply.shape[1:], bf16)
            reply_lse[s] = jnp.full(reply_lse.shape[1:], DEAD, f32)

    for half in range(1, HALVES):
        run(order_own, fold_own, bias_own, mixed_own.at[half], lse_own.at[half], half)

    filler = jnp.zeros((LANES - SUB, LANES), f32)
    gains = [
        jnp.where(me == side_of, gain_mine[...], gain_theirs[...]).reshape(1, side).astype(f32)
        for side_of in range(2)
    ]
    give = []
    for half in range(HALVES):
        for s in range(2):
            @pl.when(sides[s][1])
            def _(s=s, half=half):
                for copy in answer(s, half):
                    copy.wait_recv()
        levels = [
            jnp.concatenate(
                [
                    jnp.concatenate(
                        [reply_lse[s, half, :, b * LANES : (b + 1) * LANES], filler], axis=0
                    ).T
                    for b in range(padded // LANES)
                ],
                axis=0,
            )[:piece]
            for s in range(2)
        ]
        attended = []
        for h in range(heads):
            low, high = levels[0][:, h : h + 1], levels[1][:, h : h + 1]
            own = lse_own[half, h]
            top = jnp.maximum(own, jnp.maximum(low, high))
            share_low, share_high = jnp.exp(low - top), jnp.exp(high - top)
            share_own = jnp.exp(own - top)
            total = share_low + share_high + share_own
            summed = (
                share_own * values(mixed_own.at[half], h)
                + share_low * reply[0, half, h].astype(f32)
                + share_high * reply[1, half, h].astype(f32)
            )
            attended.append((summed * (1.0 / total)).astype(bf16))
        updated = nodes[2, half * piece : (half + 1) * piece].astype(f32) + jnp.dot(
            jnp.concatenate(attended, axis=1), out_w[...], preferred_element_type=f32
        )
        mean = jnp.sum(updated, axis=1, keepdims=True) / width
        variance = jnp.sum(updated * updated, axis=1, keepdims=True) / width - mean * mean
        result = (updated - mean) * lax.rsqrt(variance + EPSILON)
        for b in range(2):
            block_out = (result[:, b * side : (b + 1) * side] * gains[b]).astype(bf16)
            normed[half, b] = block_out
            at = pl.multiple_of(me * part + half * piece, piece)
            @pl.when(me == b)
            def _(block_out=block_out, at=at):
                out_ref[pl.ds(at, piece), :] = block_out
        give.append(remote(
            REPLY + 4 * HALVES + half, normed.at[half, other], landed.at[half], partner
        ))
        give[half].start()

    for copy in shared:
        copy.wait_send()
    for s in range(2):
        @pl.when(sides[s][1])
        def _(s=s):
            for copy in request(s):
                copy.wait_send()

        @pl.when(sides[s][3])
        def _(s=s):
            for half in range(HALVES):
                for copy in answer(s, half):
                    copy.wait_send()
    for half, copy in enumerate(give):
        copy.wait()
        at = pl.multiple_of(other * part + half * piece, piece)
        out_ref[pl.ds(at, piece), :] = landed[half]


def shards(
    grid_latent,
    mesh_latent,
    neighbours,
    edge_bias,
    query_weight,
    key_weight,
    value_weight,
    out_weight,
    norm_gain,
):
    band, width = grid_latent.shape
    count, slots = neighbours.shape
    part = count // 2
    cols = width // LANES
    heads = width // HEAD_DIM
    split = heads // 2
    side = width // 2
    chunks = part * slots // LANES
    piece = part // HALVES
    padded = -(-piece // LANES) * LANES
    far = pl.BlockSpec(memory_space=pltpu.HBM)
    copies = REPLY + 5 * HALVES
    bf16, f32, i32 = jnp.bfloat16, jnp.float32, jnp.int32
    return pl.pallas_call(
        body,
        name="attend",
        out_shape=pltpu.VMEM((count, side), bf16),
        in_specs=[far] * 9,
        out_specs=pl.BlockSpec(memory_space=pltpu.VMEM),
        scratch_shapes=[
            pltpu.VMEM((band * cols, LANES), f32),
            pltpu.VMEM((2, PIECE, width), bf16),
            pltpu.VMEM((GROUP * LANES * cols, LANES), f32),
            pltpu.VMEM((piece * slots, width), bf16),
            pltpu.VMEM((2, width, side), bf16),
            pltpu.VMEM((2, width, side), bf16),
            pltpu.VMEM((2, width, side), bf16),
            pltpu.VMEM((width, width), bf16),
            pltpu.VMEM((side,), bf16),
            pltpu.VMEM((side,), bf16),
            pltpu.VMEM((slots, count), i32),
            pltpu.VMEM((split * slots, count), bf16),
            pltpu.VMEM((3, 2 * chunks, LANES), i32),
            pltpu.VMEM((3, 2, split, chunks, LANES), bf16),
            pltpu.VMEM((3, part, width), bf16),
            pltpu.VMEM((2, chunks, LANES), i32),
            pltpu.SMEM((chunks, LANES), i32),
            pltpu.SMEM((chunks, LANES), i32),
            pltpu.SMEM((chunks, LANES), i32),
            pltpu.VMEM((3, 2, split, chunks, LANES), bf16),
            pltpu.VMEM((heads * chunks, LANES), f32),
            pltpu.VMEM((heads * chunks, LANES), f32),
            pltpu.VMEM((heads, part, width), f32),
            pltpu.VMEM((heads, part, width), f32),
            pltpu.VMEM((heads * piece, LANES), f32),
            pltpu.VMEM((heads * piece, LANES), bf16),
            pltpu.VMEM((heads, piece, width), f32),
            pltpu.VMEM((heads, padded, LANES), f32),
            pltpu.VMEM((HALVES, heads, piece, width), f32),
            pltpu.VMEM((HALVES, heads, piece, LANES), f32),
            pltpu.VMEM((2, HALVES, heads, piece, HEAD_DIM), bf16),
            pltpu.VMEM((2, HALVES, SUB, padded), f32),
            pltpu.VMEM((2, HALVES, heads, piece, HEAD_DIM), bf16),
            pltpu.VMEM((2, HALVES, SUB, padded), f32),
            pltpu.VMEM((HALVES, 2, piece, side), bf16),
            pltpu.VMEM((HALVES, piece, side), bf16),
            pltpu.SemaphoreType.DMA((2,)),
            pltpu.SemaphoreType.DMA((8,)),
            pltpu.SemaphoreType.DMA((3,)),
            pltpu.SemaphoreType.DMA((copies,)),
            pltpu.SemaphoreType.DMA((copies,)),
        ],
        compiler_params=pltpu.CompilerParams(
            collective_id=0, has_side_effects=True, vmem_limit_bytes=56 * 1024 * 1024
        ),
    )(
        grid_latent, mesh_latent, neighbours.T, edge_bias.T,
        query_weight, key_weight, value_weight, out_weight, norm_gain,
    )


def solution(mesh):
    in_specs = (
        P("lat", None),
        P("lat", None),
        P("lat", None),
        P("lat", "head"),
        P(None, "head"),
        P(None, "head"),
        P(None, "head"),
        P("head", None),
        P("head"),
    )
    out_specs = P("lat", "head")
    return jax.shard_map(shards, mesh=mesh, in_specs=in_specs, out_specs=out_specs, check_vma=False)
```
